512 devices in a mesh: dp: 8 (over y_hi, core), ep: 64 (over x, y_lo, z).
Axes of the slice: x: 4, y: 8 (y_hi: 4, y_lo: 2; y = y_hi * 2 + y_lo), z: 8, core: 2. Of those that a mesh axis runs over, the one named last changes fastest.
Arguments:
- hidden_in: bfloat16 [12288, 4096], P(('dp', 'ep')), may hold values from -6 to 6
- expert_ids: int32 [12288, 2], P(('dp', 'ep')), may hold values from 0 to 63, all different within a row; in each aligned block of 24 rows (0 to 23, 24 to 47, ...) at most 2 rows name the same one
- route_logits: float32 [12288, 64], P(('dp', 'ep')), may hold values from -10 to 10
- first_weight: bfloat16 [64, 4096, 1024], P('ep', None, 'dp'), may hold values from -0.09375 to 0.09375
- second_weight: bfloat16 [64, 1024, 4096], P('ep', None, 'dp'), may hold values from -0.1875 to 0.1875
- queries: bfloat16 [12288, 2048], P(('dp', 'ep')), may hold values from -140 to 140
- span_keys: bfloat16 [12288, 2048], P(('dp', 'ep')), may hold values from -7 to 7
- span_values: bfloat16 [12288, 2048], P(('dp', 'ep')), may hold values from -6 to 6
- cache_keys: bfloat16 [512, 72, 2048], P(('dp', 'ep')), may hold values from -6 to 6
- cache_values: bfloat16 [512, 72, 2048], P(('dp', 'ep')), may hold values from -6 to 6
- valid_frames: int32 [512], P(('dp', 'ep')), may hold values from 1 to 3
Outputs:
- mixed: bfloat16 [12288, 4096], P(('dp', 'ep'))
- attended: bfloat16 [12288, 2048], P(('dp', 'ep'))
The draws below stay inside these ranges and needn't reach their ends.
Inputs may be any that keep to these rules, and one draw needn't show every extreme that they name: `expert_ids`: each token names two different experts. In the rows of one device (24 rows) no expert is named more than 2 times, a bound that some block reaches.
All inputs are finite; a program needn't handle non-finite values.
Results may differ from the reference program's by a relative error of at most 0.0057.
Values may be sent and summed in bfloat16 or wider, within the bound.
A program may use at most 128 MiB of HBM per device.

```python
import math
import jax
import jax.numpy as jnp
import numpy as np
from jax import lax

D = 4096
FFN = 1024
HEADS = 16
HEAD_DIM = 128
TOK = 24
FRAME_TOK = 24
CFRAMES = 3
CACHE_TOK = 72
EXPERTS = 64
STREAMS = 512
TOKENS = 12288
CAP = 2


def query_key_pair(key):
    width = HEADS * HEAD_DIM
    key_rows = jnp.clip(jax.random.normal(jax.random.fold_in(key, 101), (TOKENS, width), jnp.float32), -6.0, 6.0)
    query_rows = jnp.clip(jax.random.normal(jax.random.fold_in(key, 202), (TOKENS, width), jnp.float32), -6.0, 6.0)
    return (query_rows, key_rows)


def draw_queries(key, part):
    query_rows, key_rows = query_key_pair(key)
    return query_rows.astype(jnp.bfloat16)


def draw_span_keys(key, part):
    query_rows, key_rows = query_key_pair(key)
    return key_rows.astype(jnp.bfloat16)


def set_ends(entries, own_key, low, largest):
    longest = entries.shape.index(max(entries.shape))
    spots = []
    for shift in (0, 1):
        where = [jax.random.randint(jax.random.fold_in(own_key, axis), (), 0, length) for axis, length in enumerate(entries.shape)]
        where[longest] = (where[longest] + shift) % entries.shape[longest]
        spots.append(tuple(where))
    return entries.at[spots[0]].set(low).at[spots[1]].set(largest)


def steps_of(stream_key, dims, pieces, low, high):
    loudness, own = 1.0, jax.random.fold_in(stream_key, 6)
    for dim, shards_of in pieces:
        steps = jnp.exp(jax.random.uniform(jax.random.fold_in(own, dim), (shards_of,), jnp.float32, low / len(pieces), high / len(pieces)))
        loudness = loudness * jnp.repeat(steps, dims[dim] // shards_of).reshape([-1 if axis == dim else 1 for axis in range(len(dims))])
    return loudness


def assign_block(stream_key, own, number, rows, count, top, reach, lean):
    ranking = jax.random.permutation(stream_key, count)
    crowded, ordinary = load_shares(count, rows * top, reach, lean, True), load_shares(count, rows * top, reach, lean, False)
    places = jnp.arange(count)

    def named(lengths, offset_by):
        used = int((lengths > 0).sum())
        fixed = max(1, used // 4)
        passed = fixed + (places - fixed + offset_by * (used - fixed)) % max(1, count - fixed)
        return jnp.zeros((count,), jnp.int32).at[ranking[jnp.where(places < fixed, places, passed)]].set(jnp.asarray(lengths, jnp.int32))

    lengths = jnp.where(number % 4 == 0, named(crowded, number // 4), named(ordinary, number - number // 4 - 1))
    mixed = jax.random.permutation(jax.random.fold_in(own, 3), count)
    giver, receiver = mixed[0:count // 2 * 2:2], mixed[1:count // 2 * 2:2]
    margin = jnp.minimum(lengths[giver] - 1, reach - lengths[receiver]) // 2
    margin = jnp.where((giver == ranking[0]) | (receiver == ranking[0]) | (lengths[receiver] == 0), 0, jnp.maximum(margin, 0))
    passed = jax.random.randint(jax.random.fold_in(own, 4), (count // 2,), 0, 1 << 20) % (margin + 1)
    lengths = lengths.at[giver].add(-passed).at[receiver].add(passed)
    members = jnp.searchsorted(jnp.cumsum(lengths), jnp.arange(rows * top), side="right").astype(jnp.int32)
    listing = members.reshape(top, rows).T
    listing = listing[jax.random.permutation(jax.random.fold_in(own, 1), rows)]
    offset_by = jax.random.randint(jax.random.fold_in(own, 2), (rows, 1), 0, top)
    return jnp.take_along_axis(listing, (jnp.arange(top)[None, :] + offset_by) % top, axis=1)


def load_shares(amount, total, bound, lean, full):
    portions = [(1 << 20) // math.isqrt(rank ** lean) + 1 for rank in range(1, amount + 1)]
    largest = bound if full else min(bound, max(-(-total // amount), total * portions[0] // sum(portions)))
    least = 1 if total - largest >= amount - 1 else 0
    given, surplus = [largest] + [least] * (amount - 1), total - largest - least * (amount - 1)
    while surplus > 0:
        candidates = [i for i in range(1, amount) if given[i] < largest] or [i for i in range(1, amount) if given[i] < bound]
        pool, left = sum([portions[i] for i in candidates]), surplus
        for i in candidates:
            extra = min(bound - given[i], max(1, left * portions[i] // pool), surplus)
            given[i] = given[i] + extra
            surplus = surplus - extra
    return np.array(given)


def centred(key, extent, deviation, limit, pieces=(), kind=jnp.bfloat16):
    array = deviation * jax.random.normal(key, extent, jnp.float32)
    if pieces:
        array = array * steps_of(key, extent, pieces, -0.22, 0.18)
    return jnp.clip(array, -limit, limit).astype(kind)


def setup_inputs(seed: int = 0) -> dict:
    key_list = jax.random.split(jax.random.key(seed), 12)
    hidden_in = centred(key_list[0], (TOKENS, D), 1.0, 6.0, ((0, 512),))
    expert_ids_keys = jax.random.split(jax.random.fold_in(key_list[1], 1), TOKENS // TOK)
    expert_ids_turns = jax.random.permutation(jax.random.fold_in(key_list[1], 3), TOKENS // TOK)
    expert_ids = jax.vmap(lambda own, number: assign_block(jax.random.fold_in(key_list[1], 2), own, number, TOK, EXPERTS, 2, CAP, 2))(expert_ids_keys, expert_ids_turns).reshape((TOKENS, 2))
    route_logits = centred(key_list[2], (TOKENS, EXPERTS), 2.0, 10.0, ((0, 512),), jnp.float32)
    first_weight = centred(key_list[3], (EXPERTS, D, FFN), D ** -0.5, 0.09375, ((0, 64), (2, 8)))
    second_weight = centred(key_list[4], (EXPERTS, FFN, D), FFN ** -0.5, 0.1875, ((0, 64), (2, 8)))
    queries = draw_queries(jax.random.fold_in(key_list[11], 71), 0)
    span_keys = draw_span_keys(jax.random.fold_in(key_list[11], 71), 0)
    span_values = centred(key_list[7], (TOKENS, HEADS * HEAD_DIM), 1.0, 6.0, ((0, 512),))
    cache_keys = centred(key_list[8], (STREAMS, CACHE_TOK, HEADS * HEAD_DIM), 1.0, 6.0, ((0, 512),))
    cache_values = centred(key_list[9], (STREAMS, CACHE_TOK, HEADS * HEAD_DIM), 1.0, 6.0, ((0, 512),))
    valid_frames = set_ends(jax.random.randint(key_list[10], (STREAMS,), 1, CFRAMES + 1), jax.random.fold_in(key_list[10], 1), 1, CFRAMES).astype(jnp.int32)
    return dict(hidden_in=hidden_in, expert_ids=expert_ids, route_logits=route_logits, first_weight=first_weight, second_weight=second_weight, queries=queries, span_keys=span_keys, span_values=span_values, cache_keys=cache_keys, cache_values=cache_values, valid_frames=valid_frames)


def activate(pre):
    return jax.nn.gelu(pre, approximate=True).astype(jnp.bfloat16)

def attend(queries, span_keys, span_values, cache_keys, cache_values, valid_count):
    token_count = queries.shape[0]
    cache_len = cache_keys.shape[0]
    key_rows = jnp.concatenate([cache_keys, span_keys], axis=0)
    value_rows = jnp.concatenate([cache_values, span_values], axis=0)
    query_heads = queries.reshape(token_count, HEADS, HEAD_DIM).astype(jnp.float32)
    key_heads = key_rows.reshape(-1, HEADS, HEAD_DIM).astype(jnp.float32)
    value_heads = value_rows.reshape(-1, HEADS, HEAD_DIM).astype(jnp.float32)
    scores = jnp.einsum('thd,khd->htk', query_heads, key_heads) * (1.0 / math.sqrt(HEAD_DIM))
    position = jnp.arange(key_rows.shape[0], dtype=jnp.int32)
    usable = (position >= cache_len) | (position // FRAME_TOK < valid_count)
    scores = jnp.where(usable[None, None, :], scores, -1e+30)
    row_max = lax.optimization_barrier(jnp.max(scores, axis=2, keepdims=True))
    weights = jnp.exp(scores - row_max)
    weights = (weights / lax.optimization_barrier(jnp.sum(weights, axis=2, keepdims=True))).astype(jnp.bfloat16)
    result = jnp.einsum('htk,khd->thd', weights.astype(jnp.float32), value_heads)
    return result.astype(jnp.bfloat16).reshape(token_count, HEADS * HEAD_DIM)

def block_slots(expert_ids):
    assigned = TOK * 2
    blocks = expert_ids.reshape(STREAMS, assigned)
    row_ids = lax.broadcasted_iota(jnp.int32, (assigned, assigned), 0)
    col_ids = lax.broadcasted_iota(jnp.int32, (assigned, assigned), 1)

    def per_block(flat_ids):
        same_expert = (flat_ids[:, None] == flat_ids[None, :]) & (col_ids < row_ids)
        return lax.optimization_barrier(jnp.sum(same_expert.astype(jnp.int32), axis=1))
    return jax.vmap(per_block)(blocks).reshape(TOKENS, 2)

def reference(hidden_in, expert_ids, route_logits, first_weight, second_weight, queries, span_keys, span_values, cache_keys, cache_values, valid_frames):
    slots = block_slots(expert_ids)
    token_index = jnp.arange(TOKENS, dtype=jnp.int32)
    stream_of = token_index // TOK
    rows_at = (stream_of[:, None] * CAP + slots).astype(jnp.int32)
    slot_table = jnp.full((EXPERTS, STREAMS * CAP), TOKENS, jnp.int32)
    slot_table = slot_table.at[expert_ids, rows_at].set(jnp.broadcast_to(token_index[:, None], (TOKENS, 2)))
    padded = jnp.concatenate([hidden_in, jnp.zeros((1, D), jnp.bfloat16)], axis=0)

    def apply_expert(operands):
        first_matrix, second_matrix, index_row = operands
        expert_rows = padded[index_row]
        hidden = activate(jnp.dot(expert_rows, first_matrix, preferred_element_type=jnp.float32))
        return jnp.dot(hidden, second_matrix, preferred_element_type=jnp.float32).astype(jnp.bfloat16)
    expert_outs = lax.map(apply_expert, (first_weight, second_weight, slot_table))
    chosen = jnp.take_along_axis(route_logits, expert_ids, axis=1)
    gates = jax.nn.softmax(chosen, axis=1)
    running = jnp.zeros((TOKENS, D), jnp.float32)
    for column in range(2):
        picked = expert_outs[expert_ids[:, column], rows_at[:, column]].astype(jnp.float32)
        running = running + gates[:, column:column + 1] * picked
    mixed = running.astype(jnp.bfloat16)
    width = HEADS * HEAD_DIM
    attended = jax.vmap(attend)(queries.reshape(STREAMS, TOK, width), span_keys.reshape(STREAMS, TOK, width), span_values.reshape(STREAMS, TOK, width), cache_keys, cache_values, valid_frames).reshape(TOKENS, width)
    return (mixed, attended)
```

```python
import functools
import math

import jax
import jax.numpy as jnp
from jax import lax
from jax.experimental import pallas as pl
from jax.experimental.pallas import tpu as pltpu
from jax.sharding import PartitionSpec as P

HEAD_DIM = 128
FRAME_TOK = 24
MESH = pl.DeviceIdType.MESH
F32, BF16, I32 = jnp.float32, jnp.bfloat16, jnp.int32
NQ = 4
NC = 2
NZ = 8
PAD = 32


def iota(shape, axis):
    return lax.broadcasted_iota(I32, shape, axis)


def kernel(
    hid, ids, logits, w1, w2, qr, sk, sv, ck, cv, vf,
    mixed, attended,
    tok, disp, rows, w1all, w2all, act, out, ret, meta, mix_send, mix_recv, aperm,
    z_send, z_recv, u_send, u_recv, w_send, w_recv, s_send, s_recv, a_send, a_recv,
    r_send, r_recv, m_send, m_recv, x_send, x_recv,
):
    tokens, width = hid.shape
    hidden_cols = w1.shape[1]
    out_cols = w2.shape[1]
    half = width // 2
    ep = lax.axis_index("ep")
    dp = lax.axis_index("dp")
    peers = lax.axis_size("ep")
    nu = peers // NZ
    u, z = ep // NZ, lax.rem(ep, NZ)
    q, c = dp // NC, lax.rem(dp, NC)
    zp, zm = lax.rem(z + 1, NZ), lax.rem(z + NZ - 1, NZ)
    qp, qm, qo = lax.rem(q + 1, NQ), lax.rem(q + 3, NQ), lax.rem(q + 2, NQ)
    at_zp, at_zm = {"ep": u * NZ + zp}, {"ep": u * NZ + zm}
    at_qp, at_qm, at_qo = {"dp": qp * NC + c}, {"dp": qm * NC + c}, {"dp": qo * NC + c}
    sibling = {"dp": q * NC + (1 - c)}

    def remote(src, dst, send, recv, to):
        return pltpu.make_async_remote_copy(
            src_ref=src, dst_ref=dst, send_sem=send, recv_sem=recv, device_id=to, device_id_type=MESH
        )

    barrier = pltpu.get_barrier_semaphore()
    for to in (at_qp, at_qm, at_qo, sibling):
        pl.semaphore_signal(barrier, inc=1, device_id=to, device_id_type=MESH)

    def greet(i, carry):
        pl.semaphore_signal(
            barrier, inc=1, device_id={"ep": lax.rem(ep + i, peers)}, device_id_type=MESH
        )
        return carry

    lax.fori_loop(1, peers, greet, 0)

    ids_f = ids[...].astype(F32)
    first, second = ids_f[:, 0:1], ids_f[:, 1:2]
    wide = NZ * PAD
    lane, sub = iota((tokens, wide), 1), iota((tokens, wide), 0)
    first_row = jnp.sum(jnp.where(lane == sub, first, 0.0), axis=0, keepdims=True)
    second_row = jnp.sum(jnp.where(lane == sub, second, 0.0), axis=0, keepdims=True)
    ahead = (sub < lane) & (lane < tokens)

    def row_places(row):
        same = (first == row).astype(F32) + (second == row).astype(F32)
        slot = jnp.sum(jnp.where(ahead, same, 0.0), axis=0, keepdims=True)
        lanes = iota((1, wide), 1)
        return jnp.where(lanes < tokens, row * 2.0 + slot + 1.0, 0.0)

    def col_places(col):
        same = (col == first_row).astype(F32) + (col == second_row).astype(F32)
        slot = jnp.sum(jnp.where(lane < sub, same, 0.0), axis=1, keepdims=True)
        return col * 2.0 + slot

    place_rows = (row_places(first_row), row_places(second_row))
    place_cols = (col_places(first), col_places(second))
    expert_lane = iota(logits.shape, 1).astype(F32)
    chosen = [
        jnp.sum(jnp.where(expert_lane == col, logits[...], 0.0), axis=1, keepdims=True)
        for col in (first, second)
    ]
    top = jnp.maximum(chosen[0], chosen[1])
    weight = [jnp.exp(x - top) for x in chosen]
    total = weight[0] + weight[1]
    gates = [x / total for x in weight]
    lanes = iota((tokens, 128), 1)
    record = jnp.zeros((tokens, 128), F32)
    for k, value in enumerate((*place_cols, *gates)):
        record = jnp.where(lanes == k, value, record)
    meta[q] = record
    tok[0, 0:tokens, :] = hid[...]
    tail_rows = PAD - tokens
    tail_sub = iota((tail_rows, wide), 0)
    tail = jnp.where(tail_sub == 0, place_rows[0], jnp.where(tail_sub == 1, place_rows[1], 0.0))
    tok[0, tokens:PAD, :] = jnp.zeros((tail_rows, width), BF16)
    tok[0, tokens:PAD, 0:wide] = tail.astype(BF16)

    pl.semaphore_wait(barrier, NQ + peers - 1)

    tops, bottoms = pl.ds(0, half), pl.ds(half, half)
    mine = q * NC + c

    def w1_copy(src, shard, part, sems, number, to):
        return remote(src, w1all.at[shard, part], sems[0].at[number], sems[1].at[number], to)

    w_sems = (w_send, w_recv)
    from_m, from_p, from_o = qm * NC + c, qp * NC + c, qo * NC + c
    w_copies = [
        w1_copy(w1.at[tops], mine, tops, w_sems, 0, at_qp),
        w1_copy(w1.at[bottoms], mine, bottoms, w_sems, 1, at_qm),
        w1_copy(w1.at[bottoms], mine, bottoms, w_sems, 2, at_qp),
        w1_copy(w1.at[tops], mine, tops, w_sems, 3, at_qm),
    ]
    for copy in w_copies:
        copy.start()

    def z_copy(src, dst, number, to, part=None):
        a, b = (tok.at[src], tok.at[dst]) if part is None else (tok.at[src, part], tok.at[dst, part])
        return remote(a, b, z_send.at[number], z_recv.at[number], to)

    low, high = pl.ds(0, PAD // 2), pl.ds(PAD // 2, PAD // 2)
    down = [z_copy(0, 1, 0, at_zm), z_copy(1, 2, 1, at_zm), z_copy(2, 3, 2, at_zm), z_copy(3, 4, 3, at_zm, low)]
    up = [z_copy(0, 7, 4, at_zp), z_copy(7, 6, 5, at_zp), z_copy(6, 5, 6, at_zp), z_copy(5, 4, 7, at_zp, high)]
    down[0].start()
    up[0].start()

    s_sems = (s_send, s_recv)
    other = q * NC + (1 - c)
    s_copies = [
        remote(w2, w2all.at[c], s_send.at[8], s_recv.at[8], sibling),
        w1_copy(w1.at[tops], mine, tops, s_sems, 0, sibling),
        w1_copy(w1.at[bottoms], mine, bottoms, s_sems, 1, sibling),
    ]
    for copy in s_copies:
        copy.start()
    m_copies = [
        remote(meta.at[q], meta.at[q], m_send.at[i], m_recv.at[i], to)
        for i, to in enumerate((at_qp, at_qm, at_qo))
    ]
    for copy in m_copies:
        copy.start()
    w1all[mine] = w1[...]
    w2all[c] = w2[...]

    cache_len = ck.shape[0]
    frame = iota((tokens, cache_len), 1)
    usable = frame < vf[0] * FRAME_TOK
    scale = 1.0 / math.sqrt(HEAD_DIM)
    heads = qr.shape[1] // HEAD_DIM

    def head(h, carry):
        cols = pl.ds(pl.multiple_of(h * HEAD_DIM, HEAD_DIM), HEAD_DIM)
        query = qr[:, cols]
        contract = (((1,), (1,)), ((), ()))
        old = lax.dot_general(query, ck[:, cols], contract, preferred_element_type=F32) * scale
        new = lax.dot_general(query, sk[:, cols], contract, preferred_element_type=F32) * scale
        old = jnp.where(usable, old, -1e30)
        peak = jnp.maximum(jnp.max(old, axis=1, keepdims=True), jnp.max(new, axis=1, keepdims=True))
        old, new = jnp.exp(old - peak), jnp.exp(new - peak)
        norm = jnp.sum(old, axis=1, keepdims=True) + jnp.sum(new, axis=1, keepdims=True)
        old, new = (old / norm).astype(BF16), (new / norm).astype(BF16)
        result = jnp.dot(old, cv[:, cols], preferred_element_type=F32)
        result += jnp.dot(new, sv[:, cols], preferred_element_type=F32)
        attended[:, cols] = result.astype(BF16)
        return carry

    per_step = heads // 4
    for step in range(4):
        lax.fori_loop(step * per_step, (step + 1) * per_step, head, 0)
        down[step].wait_recv()
        up[step].wait_recv()
        if step < 3:
            down[step + 1].start()
            up[step + 1].start()

    lanes = iota((1, wide), 1)
    place = [jnp.zeros((1, wide), F32), jnp.zeros((1, wide), F32)]
    for r in range(NZ):
        block = tok[r, tokens:PAD, 0:wide].astype(F32)
        if r:
            block = pltpu.roll(block, r * PAD, 1)
        for k in range(2):
            place[k] = place[k] + block[k : k + 1, :]
    picks_rows = nu * NZ * 2
    row, lane = iota((picks_rows, wide), 0), iota((picks_rows, wide), 1)
    wanted = ((row // (NZ * 2)) * NZ + z) * 2 + row % 2 + 1
    wanted_f = wanted.astype(F32)
    hit = (place[0] == wanted_f) | (place[1] == wanted_f)
    hit = hit & (lane // PAD == (row % (NZ * 2)) // 2)
    chooser = jnp.where(hit, 1.0, 0.0).astype(BF16)
    step_cols = min(512, width)

    def select(i, carry):
        cols = pl.ds(pl.multiple_of(i * step_cols, step_cols), step_cols)
        block = tok[:, :, cols].reshape(wide, step_cols)
        picked = jnp.dot(chooser, block, preferred_element_type=F32)
        disp[:, :, cols] = picked.astype(BF16).reshape(nu, NZ * 2, step_cols)
        return carry

    lax.fori_loop(0, width // step_cols, select, 0)

    def u_copy(i):
        to = lax.rem(u + i, nu)
        return remote(disp.at[to], rows.at[u], u_send, u_recv, {"ep": to * NZ + z})

    def start_u(i, carry):
        u_copy(i).start()
        return carry

    lax.fori_loop(1, nu, start_u, 0)
    rows[u] = disp[u]

    def w_recv_at(shard, part, number):
        return w1_copy(w1all.at[shard, part], shard, part, w_sems, number, at_qp)

    w_forward = [
        w1_copy(w1all.at[from_m, tops], from_m, tops, w_sems, 4, at_qp),
        w1_copy(w1all.at[from_p, bottoms], from_p, bottoms, w_sems, 5, at_qm),
    ]

    def to_sibling(shard, part, number):
        copy = w1_copy(w1all.at[shard, part], shard, part, s_sems, number, sibling)
        copy.start()
        s_copies.append(copy)

    w_recv_at(from_m, tops, 0).wait_recv()
    w_forward[0].start()
    to_sibling(from_m, tops, 2)
    w_recv_at(from_p, bottoms, 1).wait_recv()
    w_forward[1].start()
    to_sibling(from_p, bottoms, 3)
    w_recv_at(from_m, bottoms, 2).wait_recv()
    to_sibling(from_m, bottoms, 4)
    w_recv_at(from_p, tops, 3).wait_recv()
    to_sibling(from_p, tops, 5)

    if nu > 1:
        remote(
            disp.at[pl.ds(0, nu - 1)], rows.at[pl.ds(0, nu - 1)], u_send, u_recv, sibling
        ).wait_recv()

    def sibling_arrived(shard, part, number):
        w1_copy(w1all.at[shard, part], shard, part, s_sems, number, sibling).wait_recv()

    sib_m, sib_p, sib_o = qm * NC + 1 - c, qp * NC + 1 - c, qo * NC + 1 - c
    sibling_arrived(other, tops, 0)
    sibling_arrived(other, bottoms, 1)
    sibling_arrived(sib_m, tops, 2)
    sibling_arrived(sib_p, bottoms, 3)
    sibling_arrived(sib_m, bottoms, 4)
    sibling_arrived(sib_p, tops, 5)

    expert_rows = picks_rows

    def first_matmul(i, carry):
        ahead_by = i // NC
        ahead_by = jnp.where(ahead_by == 2, 3, jnp.where(ahead_by == 3, 2, ahead_by))
        shard = lax.rem(q + ahead_by, NQ) * NC + lax.rem(i, NC)
        pre = jnp.dot(rows[...].reshape(expert_rows, width), w1all[shard], preferred_element_type=F32)
        cols = pl.ds(pl.multiple_of(shard * hidden_cols, 128), hidden_cols)
        act[0, :, cols] = jax.nn.gelu(pre, approximate=True).astype(BF16)
        return carry

    lax.fori_loop(0, 6, first_matmul, 0)
    w_recv_at(from_o, tops, 4).wait_recv()
    to_sibling(from_o, tops, 6)
    w_recv_at(from_o, bottoms, 5).wait_recv()
    to_sibling(from_o, bottoms, 7)
    sibling_arrived(sib_o, tops, 6)
    sibling_arrived(sib_o, bottoms, 7)
    lax.fori_loop(6, 8, first_matmul, 0)

    act_half = expert_rows // 2
    tops, bottoms = pl.ds(0, act_half), pl.ds(act_half, act_half)

    def a_copy(src, dst, part, number, to):
        return remote(act.at[src, part], act.at[dst, part], a_send.at[number], a_recv.at[number], to)

    a_copies = [
        a_copy(0, 3, tops, 0, at_qp),
        a_copy(0, 1, bottoms, 1, at_qm),
        a_copy(0, 3, bottoms, 2, at_qp),
        a_copy(0, 1, tops, 3, at_qm),
        a_copy(3, 2, tops, 4, at_qp),
        a_copy(1, 2, bottoms, 5, at_qm),
    ]
    for copy in a_copies[:4]:
        copy.start()
    a_copies[0].wait_recv()
    a_copies[4].start()
    a_copies[1].wait_recv()
    a_copies[5].start()
    for copy in a_copies[2:]:
        copy.wait_recv()
    remote(w2, w2all.at[1 - c], s_send.at[8], s_recv.at[8], sibling).wait_recv()

    blocks = 4
    chunk = NQ * expert_rows // blocks
    all_hidden = act.shape[2]

    def second_matmul(i, carry):
        row = iota((chunk, NQ * expert_rows), 0) + i * chunk
        col = iota((chunk, NQ * expert_rows), 1)
        inner = col % expert_rows
        owner = (q + col // expert_rows) % NQ
        hit = (row // 8 == inner // 2) & ((row % 8) // 2 == owner) & (row % 2 == inner % 2)
        order = jnp.where(hit, 1.0, 0.0).astype(BF16)
        source = act[...].reshape(NQ * expert_rows, all_hidden)
        aperm[...] = jnp.dot(order, source, preferred_element_type=F32).astype(BF16)
        dests = pl.ds(i * (chunk // 8), chunk // 8)
        for part in range(NC):
            result = jnp.dot(aperm[...], w2all[part], preferred_element_type=F32)
            result = result.reshape(chunk // 8, 8, out_cols).astype(BF16)
            out[dests, :, part * out_cols : (part + 1) * out_cols] = result
        return carry

    lax.fori_loop(0, blocks, second_matmul, 0)

    def r_copy(i):
        to_u, r = lax.rem(u + i // NZ, nu), lax.rem(i, NZ)
        to = to_u * NZ + lax.rem(z + r, NZ)
        return remote(out.at[to_u * NZ + r], ret.at[ep], r_send, r_recv, {"ep": to})

    def start_r(i, carry):
        r_copy(i).start()
        return carry

    lax.fori_loop(1, peers, start_r, 0)
    ret[ep] = out[u * NZ]
    for copy in m_copies:
        copy.wait_recv()
    remote(
        out.at[pl.ds(0, peers - 1)], ret.at[pl.ds(0, peers - 1)], r_send, r_recv, sibling
    ).wait_recv()

    info = meta[...].reshape(NQ * tokens, 128)
    row, lane = iota((NQ * tokens, peers * 8), 0), iota((NQ * tokens, peers * 8), 1)
    held = (lane // 8) * 2 + lane % 2
    own = (lane % 8) // 2 == row // tokens
    held_f = held.astype(F32)
    mix_cols = NC * out_cols
    returned = ret[...].astype(F32).reshape(peers * 8, mix_cols).astype(BF16)
    running = jnp.zeros((NQ * tokens, mix_cols), F32)
    for k in range(2):
        hit = own & (info[:, k : k + 1] == held_f)
        pick = jnp.where(hit, 1.0, 0.0).astype(BF16)
        picked = jnp.dot(pick, returned, preferred_element_type=F32)
        running = running + info[:, 2 + k : 3 + k] * picked
    for i in range(NQ):
        mix_send[i] = running[i * tokens : (i + 1) * tokens].astype(BF16)
    x_copies = [
        remote(mix_send.at[to], mix_recv.at[q], x_send.at[i], x_recv.at[i], at)
        for i, (to, at) in enumerate(((qp, at_qp), (qm, at_qm), (qo, at_qo)))
    ]
    for copy in x_copies:
        copy.start()

    def place_cols_of(chip, block):
        mixed[:, pl.ds(pl.multiple_of(chip * mix_cols, 128), mix_cols)] = block

    place_cols_of(q, mix_send[q])
    for copy in (*w_copies, *w_forward, *down, *up, *s_copies, *m_copies, *a_copies):
        copy.wait_send()
    if nu > 1:
        remote(
            disp.at[pl.ds(0, nu - 1)], rows.at[pl.ds(0, nu - 1)], u_send, u_recv, sibling
        ).wait_send()
    remote(
        out.at[pl.ds(0, peers - 1)], ret.at[pl.ds(0, peers - 1)], r_send, r_recv, sibling
    ).wait_send()
    for copy, chip in zip(x_copies, (qm, qp, qo)):
        copy.wait_recv()
        place_cols_of(chip, mix_recv[chip])
    for copy in x_copies:
        copy.wait_send()


def shards(
    hidden_in, expert_ids, route_logits, first_weight, second_weight,
    queries, span_keys, span_values, cache_keys, cache_values, valid_frames,
):
    tokens, width = hidden_in.shape
    peers = lax.axis_size("ep")
    nu = peers // NZ
    _, _, hidden_cols = first_weight.shape
    _, all_hidden, out_cols = second_weight.shape
    mix_cols = NC * out_cols
    expert_rows = peers * 2
    vmem = pl.BlockSpec(memory_space=pltpu.VMEM)
    dma = pltpu.SemaphoreType.DMA
    return pl.pallas_call(
        kernel,
        out_shape=(
            jax.ShapeDtypeStruct((tokens, width), BF16),
            jax.ShapeDtypeStruct(queries.shape, BF16),
        ),
        in_specs=[vmem] * 10 + [pl.BlockSpec(memory_space=pltpu.SMEM)],
        out_specs=(vmem, vmem),
        scratch_shapes=[
            pltpu.VMEM((NZ, PAD, width), BF16),
            pltpu.VMEM((nu, NZ * 2, width), BF16),
            pltpu.VMEM((nu, NZ * 2, width), BF16),
            pltpu.VMEM((NQ * NC, width, hidden_cols), BF16),
            pltpu.VMEM((NC, all_hidden, out_cols), BF16),
            pltpu.VMEM((NQ, expert_rows, all_hidden), BF16),
            pltpu.VMEM((peers, 8, mix_cols), BF16),
            pltpu.VMEM((peers, 8, mix_cols), BF16),
            pltpu.VMEM((NQ, tokens, 128), F32),
            pltpu.VMEM((NQ, tokens, mix_cols), BF16),
            pltpu.VMEM((NQ, tokens, mix_cols), BF16),
            pltpu.VMEM((expert_rows, all_hidden), BF16),
            dma((8,)), dma((8,)),
            dma, dma,
            dma((6,)), dma((6,)),
            dma((9,)), dma((9,)),
            dma((6,)), dma((6,)),
            dma, dma,
            dma((3,)), dma((3,)),
            dma((3,)), dma((3,)),
        ],
        compiler_params=pltpu.CompilerParams(
            collective_id=0, has_side_effects=True, vmem_limit_bytes=60 * 1024 * 1024
        ),
    )(
        hidden_in, expert_ids, route_logits, first_weight[0], second_weight[0],
        queries, span_keys, span_values, cache_keys[0], cache_values[0], valid_frames,
    )


def solution(mesh):
    placed = (
        P(("dp", "ep"), None),
        P(("dp", "ep"), None),
        P(("dp", "ep"), None),
        P("ep", None, "dp"),
        P("ep", None, "dp"),
        P(("dp", "ep"), None),
        P(("dp", "ep"), None),
        P(("dp", "ep"), None),
        P(("dp", "ep"), None, None),
        P(("dp", "ep"), None, None),
        P(("dp", "ep")),
    )
    return jax.shard_map(
        shards,
        mesh=mesh,
        in_specs=placed,
        out_specs=(P(("dp", "ep"), None), P(("dp", "ep"), None)),
        check_vma=False,
    )
```
